128 devices in a mesh: gx: 16 (over y, z), gy: 8 (over x, core).
Axes of the slice: x: 4, y: 4, z: 4, core: 2. Of those that a mesh axis runs over, the one named last changes fastest.
Arguments:
- velocity: float32 [3, 128, 512, 384], P(None, 'gx', 'gy')
- target_profile: float32 [2, 384], replicated, may hold values from 0.5 to 1.5
- disc_turbine: int32 [128, 4], P(('gx', 'gy')), may hold values from -1 to 99, as said below
- disc_start: int32 [3, 128, 4], P(None, ('gx', 'gy')), may hold values from 0 to 256, as said below
- disc_weight: float32 [128, 4, 16, 128], P(('gx', 'gy')), may hold values from 0.2 to 1
- turbine_owner: int32 [100], replicated, may hold values from 0 to 127, as said below
- mode_flag: int32 [100], replicated, may hold values from 0 to 2
- controller_state: float32 [128, 4], P(('gx', 'gy')), may hold values from -4 to 4
Outputs:
- advanced_velocity: float32 [3, 128, 512, 384], P(None, 'gx', 'gy')
- profiles: float32 [4, 384], replicated
- thrust_setpoint: float32 [100], replicated
- controller_next: float32 [128, 4], P(('gx', 'gy'))
The draws below stay inside these ranges and needn't reach their ends.
Inputs may be any that keep to these rules, and one draw needn't show every extreme that they name: `disc_turbine`: -1 marks an empty slot; every turbine number appears in at least one slot; some device has all 4 slots filled. `disc_start`: row 0 is a cell of the device's block along the first dimension, 0 to 7; row 1 the first of 16 cells along the second, 0 to 48; row 2 the first of 128 heights, 0 to 256. `turbine_owner`: no device owns more than 4 turbines, and some device owns exactly 4.
All inputs are finite; a program needn't handle non-finite values.
Results may differ from the reference program's by a relative error of at most 0.00013.
Values sent between devices are 32-bit elements; how exact they have to be, the bound alone decides.
No kernel may reach another device: no remote copies, remote signals or barrier semaphores. Data moves between devices by JAX's collectives and lax.ppermute only.
A program may use at most 128 MiB of HBM per device.

```python
import math
import jax
import jax.numpy as jnp
from jax import lax

CX = 8
CY = 64
NZ = 384
STEPS = 4
NT = 100
SLOTS = 4
OWN = 4
TY = 16
TZ = 128
NX = 128
NY = 512
N_GX = 16
N_GY = 8


def draw_velocity(key, part):
    key_u, key_v, key_w = jax.random.split(key, 3)
    shape = (NX, NY, NZ)
    height = (jnp.arange(NZ, dtype=jnp.float32) + 0.5) / NZ
    mean_wind = 0.4 + 0.8 * jnp.log1p(40.0 * height) / jnp.log1p(40.0)
    along = (jnp.arange(NX, dtype=jnp.float32) + 0.5) / NX
    rough_u = jax.random.normal(key_u, shape, jnp.float32)
    rough_v = jax.random.normal(key_v, shape, jnp.float32)
    rough_w = jax.random.normal(key_w, shape, jnp.float32)
    amplitude = 0.1 * (1.0 + 2.0 * along)[:, None, None]
    smooth_part = jnp.zeros((1, NY, 1), jnp.float32)
    component_u = mean_wind[None, None, :] + smooth_part + amplitude * rough_u
    component_v = amplitude * rough_v
    component_w = 0.5 * amplitude * rough_w
    return jnp.stack([component_u, component_v, component_w]).astype(jnp.float32)


def draw_disc_turbine(key, part):
    devices = N_GX * N_GY
    total_slots = devices * SLOTS
    key_order, key_heavy = jax.random.split(jax.random.fold_in(key, 7))
    position = jax.random.permutation(key_order, total_slots).astype(jnp.int32)
    heavy_rank = jax.random.permutation(key_heavy, devices).astype(jnp.int32)
    heavy_device = heavy_rank < max(1, devices // 4)
    heavy_slot = jnp.repeat(heavy_device, SLOTS)
    live_slot = (position < NT) | heavy_slot
    return jnp.where(live_slot, position % NT, -1).astype(jnp.int32).reshape(devices, SLOTS)


def draw_disc_start(key, part):
    devices = N_GX * N_GY
    key_x, key_y, key_z = jax.random.split(jax.random.fold_in(key, 3), 3)
    shape = (devices, SLOTS)
    first_x = jax.random.randint(key_x, shape, 0, CX)
    first_y = jax.random.randint(key_y, shape, 0, CY - TY + 1)
    first_z = jax.random.randint(key_z, shape, 0, NZ - TZ + 1)
    return jnp.stack([first_x, first_y, first_z]).astype(jnp.int32)


def draw_turbine_owner(key, part):
    devices = N_GX * N_GY
    key_group, key_device = jax.random.split(jax.random.fold_in(key, 5))
    turbine_order = jax.random.permutation(key_group, NT).astype(jnp.int32)
    device_order = jax.random.permutation(key_device, devices).astype(jnp.int32)
    return device_order[turbine_order // OWN].astype(jnp.int32)


def set_ends(array, stream_key, least, top_value):
    longest = array.shape.index(max(array.shape))
    spots = []
    for shift in (0, 1):
        where = [jax.random.randint(jax.random.fold_in(stream_key, axis), (), 0, length) for axis, length in enumerate(array.shape)]
        where[longest] = (where[longest] + shift) % array.shape[longest]
        spots.append(tuple(where))
    return array.at[spots[0]].set(least).at[spots[1]].set(top_value)


def steps_of(rng, shape, pieces, low, high):
    level = 1.0
    for dim, parts in pieces:
        draws = jax.random.uniform(jax.random.fold_in(jax.random.fold_in(rng, 6), dim), (parts,), jnp.float32, low / len(pieces), high / len(pieces))
        level = level * jnp.repeat(jnp.exp(draws), shape[dim] // parts).reshape((-1,) + (1,) * (len(shape) - 1 - dim))
    return level


def bell_draw(stream_key, dims, deviation, bound, shards=(), kind=jnp.bfloat16):
    loudness = steps_of(stream_key, dims, shards, -0.22, 0.18) if shards else 1.0
    result = jax.random.normal(stream_key, dims, jnp.float32) * deviation * loudness
    return jnp.minimum(jnp.maximum(result, -bound), bound).astype(kind)


def setup_inputs(seed: int = 0) -> dict:
    keys = jax.random.split(jax.random.key(seed), 9)
    return {
        "velocity": draw_velocity(jax.random.fold_in(keys[8], 71), 0),
        "target_profile": jnp.clip(jax.random.uniform(keys[1], (2, NZ), jnp.float32, 0.5, 1.5), 0.5, 1.5),
        "disc_turbine": draw_disc_turbine(jax.random.fold_in(keys[8], 71), 0),
        "disc_start": draw_disc_start(jax.random.fold_in(keys[8], 71), 0),
        "disc_weight": jnp.clip(jnp.exp(math.log(1.0) - 1.609438 * jax.random.uniform(keys[4], (N_GX * N_GY, SLOTS, TY, TZ), jnp.float32) ** steps_of(keys[4], (N_GX * N_GY, SLOTS, TY, TZ), ((0, 128),), -0.2, 0.2)), 0.2, 1.0),
        "turbine_owner": draw_turbine_owner(jax.random.fold_in(keys[8], 71), 0),
        "mode_flag": set_ends(jax.random.randint(keys[6], (NT,), 0, 3), jax.random.fold_in(keys[6], 1), 0, 2).astype(jnp.int32),
        "controller_state": bell_draw(keys[7], (N_GX * N_GY, OWN), 1.0, 4.0, ((0, 128),), jnp.float32),
    }


VISCOSITY = 0.1
TIME_STEP = 0.2
RELAX_TIME = 2.0
CONTROL_STEP = 0.5
GAIN_PROPORTIONAL = 2.0
GAIN_INTEGRAL = 1.0
HIGHEST = lax.Precision.HIGHEST


def neighbours(field, direction, offset):
    if direction == 2:
        extent = field.shape[2]
        padded = jnp.pad(field, ((0, 0), (0, 0), (2, 2)))
        return padded[:, :, 2 + offset:2 + offset + extent]
    return jnp.roll(field, -offset, direction)


def derivative(field, direction):
    return (8.0 * (neighbours(field, direction, 1) - neighbours(field, direction, -1)) - (neighbours(field, direction, 2) - neighbours(field, direction, -2))) / 12.0


def tendency(velocity):
    results = []
    for component in range(3):
        field = velocity[component]
        laplacian = (neighbours(field, 0, 1) + neighbours(field, 0, -1)) + (neighbours(field, 1, 1) + neighbours(field, 1, -1)) + (neighbours(field, 2, 1) + neighbours(field, 2, -1)) - 6.0 * field
        advection = velocity[0] * derivative(field, 0) + velocity[1] * derivative(field, 1) + velocity[2] * derivative(field, 2)
        results.append(VISCOSITY * laplacian - advection)
    return jnp.stack(results)


def control_terms(mode_flag):
    rated_speed = jnp.where(mode_flag == 0, 0.7, jnp.where(mode_flag == 1, 0.9, 1.1)).astype(jnp.float32)
    bias_terms = jnp.where(mode_flag == 0, 1.0, jnp.where(mode_flag == 1, 0.0, -1.0)).astype(jnp.float32)
    return rated_speed, bias_terms


def owner_rank(turbine_owner):
    turbines = turbine_owner.shape[0]
    same_owner = turbine_owner[:, None] == turbine_owner[None, :]
    earlier = jnp.arange(turbines, dtype=jnp.int32)[None, :] < jnp.arange(turbines, dtype=jnp.int32)[:, None]
    return jnp.sum((same_owner & earlier).astype(jnp.int32), axis=1).astype(jnp.int32)


def reference(velocity, target_profile, disc_turbine, disc_start, disc_weight, turbine_owner, mode_flag, controller_state):
    devices = N_GX * N_GY
    total_slots = devices * SLOTS
    slot_turbine = disc_turbine.reshape(total_slots)
    device_index = jnp.repeat(jnp.arange(devices, dtype=jnp.int32), SLOTS)
    start_x = ((device_index // N_GY) * CX + disc_start[0].reshape(total_slots)).astype(jnp.int32)
    start_y = ((device_index % N_GY) * CY + disc_start[1].reshape(total_slots)).astype(jnp.int32)
    start_z = disc_start[2].reshape(total_slots).astype(jnp.int32)
    weights_flat = disc_weight.reshape(total_slots, TY, TZ)
    slot_onehot = (slot_turbine[:, None] == jnp.arange(NT, dtype=jnp.int32)[None, :]).astype(jnp.float32)
    disc_area = jnp.dot(jnp.sum(weights_flat, axis=(1, 2)), slot_onehot, precision=HIGHEST)
    owner_slot = owner_rank(turbine_owner)
    owner_column = (turbine_owner * OWN + owner_slot).astype(jnp.int32)
    state_flat = controller_state.reshape(devices * OWN)
    integral = state_flat[owner_column]
    rated_speed, bias_terms = control_terms(mode_flag)
    profiles = jnp.zeros((4, NZ), jnp.float32)
    thrust = jnp.zeros((NT,), jnp.float32)
    for turn_index in range(STEPS):
        streamwise = velocity[0]

        def disc_probe(slot_index):
            window_cells = lax.dynamic_slice(streamwise, (start_x[slot_index], start_y[slot_index], start_z[slot_index]), (1, TY, TZ))[0]
            return jnp.sum(weights_flat[slot_index] * window_cells)

        contribution = lax.map(disc_probe, jnp.arange(total_slots, dtype=jnp.int32))
        numerator = jnp.dot(contribution, slot_onehot, precision=HIGHEST)
        disc_speed = numerator / disc_area
        plane_sums = jnp.stack([jnp.sum(velocity[0], axis=(0, 1)), jnp.sum(velocity[1], axis=(0, 1)), jnp.sum(velocity[2], axis=(0, 1)), jnp.sum(velocity[0] * velocity[2], axis=(0, 1))])
        plane_means = plane_sums / (NX * NY)
        profiles = profiles + jnp.stack([plane_means[0], plane_means[1], plane_means[2], plane_means[3] - plane_means[0] * plane_means[2]])
        speed_error = disc_speed - rated_speed
        integral = integral + CONTROL_STEP * speed_error
        thrust = 0.1 + 0.9 * jax.nn.sigmoid(bias_terms - GAIN_PROPORTIONAL * speed_error - GAIN_INTEGRAL * integral)
        thrust_factor = 0.5 * thrust * disc_speed * jnp.abs(disc_speed)
        slot_factor = jnp.dot(slot_onehot, thrust_factor, precision=HIGHEST)

        def add_tile(slot_index, force_field):
            corner = (start_x[slot_index], start_y[slot_index], start_z[slot_index])
            previous = lax.dynamic_slice(force_field, corner, (1, TY, TZ))
            return lax.dynamic_update_slice(force_field, previous - slot_factor[slot_index] * weights_flat[slot_index][None], corner)

        force_field = lax.fori_loop(0, total_slots, add_tile, jnp.zeros((NX, NY, NZ), jnp.float32))
        nudging = (target_profile - plane_means[0:2]) / RELAX_TIME
        changes = tendency(velocity)
        velocity = jnp.stack([
            velocity[0] + TIME_STEP * (changes[0] + nudging[0][None, None, :] + force_field),
            velocity[1] + TIME_STEP * (changes[1] + nudging[1][None, None, :]),
            velocity[2] + TIME_STEP * changes[2]])
    controller_next = state_flat.at[owner_column].set(integral).reshape(devices, OWN)
    return velocity, profiles / STEPS, thrust, controller_next
```

```python
import functools

import jax
import jax.numpy as jnp
from jax import lax
from jax.experimental import pallas as pl
from jax.experimental.pallas import tpu as pltpu
from jax.sharding import Mesh
from jax.sharding import PartitionSpec as P

STEPS = 4
GX = ("gx_0", "gx_1")
GY = ("gy_0", "gy_1")
GX_GY = ("gx_0", "gx_1", "gy_0", "gy_1")
CHIPS = ("gx_0", "gx_1", "gy_0")

LANES = 128
ROWS = 16
ROW_U, ROW_V, ROW_W, ROW_UW, ROW_NUM, ROW_AREA, ROW_INT = 0, 3, 6, 9, 12, 13, 14
CHUNK = 16


def placed_spec(space):
    return pl.BlockSpec(memory_space=space)


VM = pltpu.VMEM
SM = pltpu.SMEM
ANY = pl.ANY


def sums_kernel(starts, ids, velocity, weight, integral0, payload, planes, field, sem, *, copies):
    _, nx, ny, nz = velocity.shape
    tiles = nz // LANES
    slots, tile_y, tile_z = weight.shape
    load = pltpu.make_async_copy(velocity, field, sem)
    load.start()
    for s in range(slots):
        tile = jnp.concatenate(
            [weight[s], jnp.zeros((tile_y, nz - tile_z), jnp.float32)], axis=1
        )
        tile = pltpu.roll(tile, starts[2, s], axis=1)
        plane = jnp.concatenate([tile, jnp.zeros((ny - tile_y, nz), jnp.float32)], axis=0)
        planes[s] = pltpu.roll(plane, starts[1, s], axis=0)
    load.wait()

    def add_plane(i, carry):
        out = []
        for t in range(tiles):
            lanes = slice(t * LANES, (t + 1) * LANES)
            u = field[0, i, :, lanes].reshape(ny // 8, 8, LANES)
            v = field[1, i, :, lanes].reshape(ny // 8, 8, LANES)
            w = field[2, i, :, lanes].reshape(ny // 8, 8, LANES)
            out.append(
                (
                    carry[t][0] + jnp.sum(u, axis=0),
                    carry[t][1] + jnp.sum(v, axis=0),
                    carry[t][2] + jnp.sum(w, axis=0),
                    carry[t][3] + jnp.sum(u * w, axis=0),
                )
            )
        return tuple(out)

    zero = jnp.zeros((8, LANES), jnp.float32)
    sums = lax.fori_loop(0, nx, add_plane, ((zero,) * 4,) * tiles)
    rows = [None] * ROWS
    for q, base in enumerate((ROW_U, ROW_V, ROW_W, ROW_UW)):
        for t in range(tiles):
            rows[base + t] = jnp.sum(sums[t][q], axis=0, keepdims=True)
    lane = lax.broadcasted_iota(jnp.int32, (1, LANES), 1)
    numerator = jnp.zeros((1, LANES), jnp.float32)
    area = jnp.zeros((1, LANES), jnp.float32)
    for s in range(slots):
        mine = lane == ids[0, s]
        seen = jnp.sum(planes[s] * field[0, starts[0, s]], keepdims=True)
        total = jnp.sum(weight[s], keepdims=True)
        numerator = numerator + jnp.where(mine, seen, 0.0)
        area = area + jnp.where(mine, total, 0.0)
    rows[ROW_NUM] = numerator
    rows[ROW_AREA] = area
    rows[ROW_INT] = integral0[...]
    rows[ROWS - 1] = jnp.zeros((1, LANES), jnp.float32)
    full = jnp.concatenate(rows, axis=0)
    for c in range(copies):
        payload[c] = full


def step_kernel(
    starts, ids, velocity, x_low, x_high, y_low, y_high, reduced, planes, target, terms, state,
    *rest, cells, last, first, turbines, copies,
):
    if last:
        velocity_out, state_out = rest[:2]
        scratch = rest[2:]
    else:
        velocity_out, xs_low, xs_high, ys_low, ys_high, payload, state_out = rest[:7]
        scratch = rest[7:]
    padded, field, sums, sems = scratch
    _, nx, ny, nz = velocity.shape
    tiles = nz // LANES
    slots = planes.shape[0]
    loads = []
    for t in range(tiles):
        lanes = pl.ds(t * LANES, LANES)
        loads.append(
            pltpu.make_async_copy(
                velocity.at[:, :, :, lanes],
                padded.at[:, pl.ds(2, nx), t, pl.ds(8, ny), :],
                sems.at[3 * t],
            )
        )
        loads.append(
            pltpu.make_async_copy(
                x_low.at[:, :, :, lanes],
                padded.at[:, pl.ds(0, 2), t, pl.ds(8, ny), :],
                sems.at[3 * t + 1],
            )
        )
        loads.append(
            pltpu.make_async_copy(
                x_high.at[:, :, :, lanes],
                padded.at[:, pl.ds(nx + 2, 2), t, pl.ds(8, ny), :],
                sems.at[3 * t + 2],
            )
        )
    for load in loads:
        load.start()

    lane = lax.broadcasted_iota(jnp.int32, (1, LANES), 1)
    total = reduced[0] + reduced[1]
    means = total[0:12] * (1.0 / cells)
    if first:
        area = total[ROW_AREA : ROW_AREA + 1]
        integral = total[ROW_INT : ROW_INT + 1]
        profiles = jnp.zeros((12, LANES), jnp.float32)
    else:
        area = state[13:14]
        integral = state[12:13]
        profiles = state[0:12]
    live = lane < turbines
    disc_speed = total[ROW_NUM : ROW_NUM + 1] / jnp.where(live, area, 1.0)
    speed_error = disc_speed - terms[0:1]
    integral = integral + 0.5 * speed_error
    thrust = 0.1 + 0.9 * jax.nn.sigmoid(terms[1:2] - 2.0 * speed_error - integral)
    factor = 0.5 * thrust * disc_speed * jnp.abs(disc_speed)
    product = jnp.concatenate(
        [jnp.zeros((9, LANES), jnp.float32), means[0:3] * means[6:9]], axis=0
    )
    state_out[0:12] = profiles + (means - product)
    state_out[12:13] = integral
    state_out[13:14] = area
    state_out[14:15] = thrust
    state_out[15:16] = jnp.zeros((1, LANES), jnp.float32)
    push = [0.1 * (target[r : r + 1] - means[r : r + 1]) for r in range(6)]
    forces = [
        -0.2 * jnp.sum(jnp.where(lane == ids[0, s], factor, 0.0), axis=1, keepdims=True)
        for s in range(slots)
    ]

    for c in range(3):
        for i in range(nx):
            for t in range(tiles):
                lanes = slice(t * LANES, (t + 1) * LANES)
                padded[c, i + 2, t, 6:8, :] = y_low[c, i, :, lanes]
                padded[c, i + 2, t, 8 + ny : 10 + ny, :] = y_high[c, i, :, lanes]
    for load in loads:
        load.wait()

    if not last:
        sums[...] = jnp.zeros(sums.shape, jnp.float32)
    wide = lax.broadcasted_iota(jnp.int32, (CHUNK, LANES), 1)
    edge = [wide < 1, wide < 2, wide >= LANES - 1, wide >= LANES - 2]

    def plane(i, carry):
        for y in range(0, ny, CHUNK):

            def at(c, t, dx, dy):
                return padded[c, i + 2 + dx, t, pl.ds(8 + y + dy, CHUNK), :]

            speed = [[at(c, t, 0, 0) for t in range(tiles)] for c in range(3)]
            new = [[None] * tiles for _ in range(3)]
            for c in range(3):
                centre = speed[c]
                up1 = [pltpu.roll(centre[t], 1, axis=1) for t in range(tiles)]
                up2 = [pltpu.roll(centre[t], 2, axis=1) for t in range(tiles)]
                dn1 = [pltpu.roll(centre[t], LANES - 1, axis=1) for t in range(tiles)]
                dn2 = [pltpu.roll(centre[t], LANES - 2, axis=1) for t in range(tiles)]
                for t in range(tiles):
                    f = centre[t]
                    below, above = t > 0, t < tiles - 1
                    zm1 = jnp.where(edge[0], up1[t - 1] if below else 0.0, up1[t])
                    zm2 = jnp.where(edge[1], up2[t - 1] if below else 0.0, up2[t])
                    zp1 = jnp.where(edge[2], dn1[t + 1] if above else 0.0, dn1[t])
                    zp2 = jnp.where(edge[3], dn2[t + 1] if above else 0.0, dn2[t])
                    xm1, xp1 = at(c, t, -1, 0), at(c, t, 1, 0)
                    ym1, yp1 = at(c, t, 0, -1), at(c, t, 0, 1)
                    grad_x = 8.0 * (xp1 - xm1) - (at(c, t, 2, 0) - at(c, t, -2, 0))
                    grad_y = 8.0 * (yp1 - ym1) - (at(c, t, 0, 2) - at(c, t, 0, -2))
                    grad_z = 8.0 * (zp1 - zm1) - (zp2 - zm2)
                    around = (xp1 + xm1) + (yp1 + ym1) + (zp1 + zm1)
                    moved = speed[0][t] * grad_x + speed[1][t] * grad_y + speed[2][t] * grad_z
                    result = 0.88 * f + (0.02 * around - (0.2 / 12.0) * moved)
                    if c < 2:
                        result = result + push[3 * c + t]
                    new[c][t] = result
                    field[c, i, y : y + CHUNK, t * LANES : (t + 1) * LANES] = result
            if not last:
                for t in range(tiles):
                    u, v, w = new[0][t], new[1][t], new[2][t]
                    for q, value in enumerate((u, v, w, u * w)):
                        part = value[0:8]
                        for r in range(8, CHUNK, 8):
                            part = part + value[r : r + 8]
                        sums[q, t] = sums[q, t] + part
        return carry

    lax.fori_loop(0, nx, plane, 0)

    for s in range(slots):
        i = starts[0, s]
        push_s = forces[s] * planes[s]
        field[0, i] = field[0, i] + push_s
        if not last:
            along = push_s * field[2, i]
            for t in range(tiles):
                lanes = slice(t * LANES, (t + 1) * LANES)
                sums[0, t] = sums[0, t] + jnp.sum(
                    push_s[:, lanes].reshape(ny // 8, 8, LANES), axis=0
                )
                sums[3, t] = sums[3, t] + jnp.sum(
                    along[:, lanes].reshape(ny // 8, 8, LANES), axis=0
                )

    stores = [pltpu.make_async_copy(field, velocity_out, sems.at[0])]
    if not last:
        stores.append(pltpu.make_async_copy(field.at[:, pl.ds(0, 2)], xs_low, sems.at[1]))
        stores.append(pltpu.make_async_copy(field.at[:, pl.ds(nx - 2, 2)], xs_high, sems.at[2]))
    for store in stores:
        store.start()
    if not last:
        ys_low[...] = field[:, :, 0:2, :]
        ys_high[...] = field[:, :, ny - 2 : ny, :]
        rows = []
        for q in range(4):
            for t in range(tiles):
                rows.append(jnp.sum(sums[q, t], axis=0, keepdims=True))
        numerator = jnp.zeros((1, LANES), jnp.float32)
        for s in range(slots):
            seen = jnp.sum(planes[s] * field[0, starts[0, s]], keepdims=True)
            numerator = numerator + jnp.where(lane == ids[0, s], seen, 0.0)
        rows.append(numerator)
        rows.append(jnp.zeros((3, LANES), jnp.float32))
        full = jnp.concatenate(rows, axis=0)
        for k in range(copies):
            payload[k] = full
    for store in stores:
        store.wait()


def first_sums(starts, ids, velocity, weight, integral0, copies):
    _, nx, ny, nz = velocity.shape
    return pl.pallas_call(
        functools.partial(sums_kernel, copies=copies),
        out_shape=(
            jax.ShapeDtypeStruct((copies, ROWS, LANES), jnp.float32),
            jax.ShapeDtypeStruct((weight.shape[0], ny, nz), jnp.float32),
        ),
        in_specs=[placed_spec(SM), placed_spec(SM), placed_spec(ANY), placed_spec(VM), placed_spec(VM)],
        out_specs=(placed_spec(VM), placed_spec(VM)),
        scratch_shapes=[pltpu.VMEM(velocity.shape, jnp.float32), pltpu.SemaphoreType.DMA(())],
        compiler_params=pltpu.CompilerParams(vmem_limit_bytes=24 * 2**20),
        name="first_sums",
    )(starts, ids, velocity, weight, integral0)


def one_step(starts, ids, velocity, halos, reduced, planes, target, terms, state, *, cells, last, first, turbines, copies):
    _, nx, ny, nz = velocity.shape
    x_low, x_high, y_low, y_high = halos
    f32 = jnp.float32
    outs = [jax.ShapeDtypeStruct(velocity.shape, f32)]
    specs = [placed_spec(ANY)]
    if not last:
        outs += [jax.ShapeDtypeStruct((3, 2, ny, nz), f32)] * 2
        specs += [placed_spec(ANY)] * 2
        outs += [jax.ShapeDtypeStruct((3, nx, 2, nz), f32)] * 2
        specs += [placed_spec(VM)] * 2
        outs += [jax.ShapeDtypeStruct((copies, ROWS, LANES), f32)]
        specs += [placed_spec(VM)]
    outs += [jax.ShapeDtypeStruct((16, LANES), f32)]
    specs += [placed_spec(VM)]
    return pl.pallas_call(
        functools.partial(
            step_kernel, cells=cells, last=last, first=first, turbines=turbines, copies=copies
        ),
        out_shape=tuple(outs),
        in_specs=[placed_spec(SM)] * 2 + [placed_spec(ANY)] * 3 + [placed_spec(VM)] * 7,
        out_specs=tuple(specs),
        scratch_shapes=[
            pltpu.VMEM((3, nx + 4, nz // LANES, ny + 16, LANES), f32),
            pltpu.VMEM(velocity.shape, f32),
            pltpu.VMEM((4, nz // LANES, 8, LANES), f32),
            pltpu.SemaphoreType.DMA((9,)),
        ],
        compiler_params=pltpu.CompilerParams(vmem_limit_bytes=32 * 2**20),
        name="one_step",
    )(starts, ids, velocity, x_low, x_high, y_low, y_high, reduced, planes, target, terms, state)


def exchange(edges):
    def shift(block, axis, by):
        n = lax.axis_size(axis)
        return lax.ppermute(block, axis, [(i, (i + by) % n) for i in range(n)])

    x_first, x_last, y_first, y_last = edges
    return (
        shift(x_last, GX, 1),
        shift(x_first, GX, -1),
        shift(y_last, GY, 1),
        shift(y_first, GY, -1),
    )


def reduce_all(payload):
    got = lax.all_to_all(payload, CHIPS, 0, 0, tiled=True)
    mine = jnp.sum(got, axis=0)
    other = lax.ppermute(mine, "gy_1", [(0, 1), (1, 0)])
    return jnp.stack([mine, other])


def owner_rank(turbine_owner):
    turbines = turbine_owner.shape[0]
    ids = jnp.arange(turbines, dtype=jnp.int32)
    same_owner = turbine_owner[:, None] == turbine_owner[None, :]
    earlier = ids[None, :] < ids[:, None]
    return jnp.sum((same_owner & earlier).astype(jnp.int32), axis=1)


def local(
    velocity, target_profile, disc_turbine, disc_start, disc_weight, turbine_owner, mode_flag,
    controller_state,
):
    blocks_x = lax.axis_size(GX)
    blocks_y = lax.axis_size(GY)
    device_me = lax.axis_index(GX) * blocks_y + lax.axis_index(GY)
    _, nx, ny, nz = velocity.shape
    turbines = mode_flag.shape[0]
    owned = controller_state.shape[1]
    cells = float(nx * blocks_x * ny * blocks_y)
    copies = lax.axis_size(CHIPS)
    starts = disc_start[:, 0, :]
    ids = disc_turbine

    rank = owner_rank(turbine_owner)
    mine_table = (turbine_owner[:, None] == device_me) & (
        rank[:, None] == jnp.arange(owned, dtype=jnp.int32)[None, :]
    )
    held = jnp.sum(jnp.where(mine_table, controller_state[0][None, :], 0.0), axis=1)
    spare = (0, LANES - turbines)
    integral0 = jnp.pad(held, spare)[None, :]
    rated = jnp.where(mode_flag == 0, 0.7, jnp.where(mode_flag == 1, 0.9, 1.1)).astype(jnp.float32)
    bias = jnp.where(mode_flag == 0, 1.0, jnp.where(mode_flag == 1, 0.0, -1.0)).astype(jnp.float32)
    terms = jnp.stack([jnp.pad(rated, spare), jnp.pad(bias, spare)])
    target = target_profile.reshape(2 * nz // LANES, LANES)

    edges = (
        velocity[:, 0:2],
        velocity[:, nx - 2 : nx],
        velocity[:, :, 0:2],
        velocity[:, :, ny - 2 : ny],
    )
    payload, planes = first_sums(starts, ids, velocity, disc_weight[0], integral0, copies)
    state = jnp.zeros((16, LANES), jnp.float32)
    for turn in range(STEPS):
        halos = exchange(edges)
        reduced = reduce_all(payload)
        out = one_step(
            starts, ids, velocity, halos, reduced, planes, target, terms, state,
            cells=cells, last=turn == STEPS - 1, first=turn == 0, turbines=turbines, copies=copies,
        )
        velocity, state = out[0], out[-1]
        if turn < STEPS - 1:
            edges, payload = out[1:5], out[5]
    profiles = state[0:12].reshape(4, nz) / STEPS
    integral = state[12, :turbines]
    thrust = state[14, :turbines]
    updated = jnp.sum(jnp.where(mine_table, integral[:, None], 0.0), axis=0)
    controller = jnp.where(jnp.any(mine_table, axis=0), updated, controller_state[0])
    return velocity, profiles, thrust, controller[None, :]


def solution(mesh):
    torus = Mesh(mesh.devices.reshape(4, 4, 4, 2), ("gx_0", "gx_1", "gy_0", "gy_1"))
    placed = (
        P(None, GX, GY, None),
        P(),
        P(GX_GY, None),
        P(None, GX_GY, None),
        P(GX_GY, None, None, None),
        P(),
        P(),
        P(GX_GY, None),
    )
    return jax.shard_map(
        local,
        mesh=torus,
        in_specs=placed,
        out_specs=(P(None, GX, GY, None), P(), P(), P(GX_GY, None)),
        check_vma=False,
    )
```
